32 devices in a mesh: section: 2 (over x), dp: 8 (over z, y), mp: 2 (over core).
Axes of the slice: x: 2, y: 2, z: 4, core: 2. Of those that a mesh axis runs over, the one named last changes fastest.
Arguments:
- layer_inputs: bfloat16 [2, 128, 4096], P('section', None, 'mp'), may hold values from -6 to 6
- pre_act: bfloat16 [2, 128, 8192], P('section', None, 'dp'), may hold values from -6 to 6
- out_grad: bfloat16 [128, 4096], P(None, 'mp'), may hold values from -4 to 4
- w_in: bfloat16 [8, 2, 512, 4096], P('dp', 'section', None, 'mp'), may hold values from -0.09375 to 0.09375
- w_out: bfloat16 [8, 2, 512, 4096], P('dp', 'section', None, 'mp'), may hold values from -0.0625 to 0.0625
Outputs:
- in_grads: bfloat16 [2, 128, 4096], P('section', None, 'mp')
- grad_in: float32 [8, 2, 512, 4096], P('dp', 'section', None, 'mp')
- grad_out: float32 [8, 2, 512, 4096], P('dp', 'section', None, 'mp')
The draws below stay inside these ranges and needn't reach their ends.
All inputs are finite; a program needn't handle non-finite values.
Results may differ from the reference program's by a relative error of at most 0.035.
Values may be sent and summed in bfloat16 or wider, within the bound.
A program may use at most 64 MiB of HBM per device.

```python
import jax
import jax.numpy as jnp
from jax import lax

D = 4096
FF = 8192
TOKS = 128
SECTIONS = 2
FB = 512
N_SECTION = 2
N_DP = 8
N_MP = 2


def block_levels(rng, shape, shards, low, largest):
    gain, own = 1.0, jax.random.fold_in(rng, 6)
    for dim, blocks in shards:
        draws = jnp.exp(jax.random.uniform(jax.random.fold_in(own, dim), (blocks,), jnp.float32, low / len(shards), largest / len(shards)))
        gain = gain * jnp.repeat(draws, shape[dim] // blocks).reshape([-1 if axis == dim else 1 for axis in range(len(shape))])
    return gain


def centred(stream_key, extent, scale, bound, split=(), held_as=jnp.bfloat16):
    level = block_levels(stream_key, extent, split, -0.22, 0.18) if split else 1.0
    entries = jax.random.normal(stream_key, extent, jnp.float32) * scale * level
    return jnp.minimum(jnp.maximum(entries, -bound), bound).astype(held_as)


def setup_inputs(seed: int = 0) -> dict:
    streams_of = jax.random.split(jax.random.key(seed), 6)
    layer_inputs = centred(streams_of[0], (SECTIONS, TOKS, D), 1.0, 6.0, ((0, 2), (2, 2)))
    pre_act = centred(streams_of[1], (SECTIONS, TOKS, FF), 1.0, 6.0, ((0, 2), (2, 8)))
    out_grad = centred(streams_of[2], (TOKS, D), 0.3, 4.0, ((1, 2),))
    w_in = centred(streams_of[3], (N_DP, N_SECTION, FB, D), D ** -0.5, 0.09375, ((0, 8), (1, 2), (3, 2)))
    w_out = centred(streams_of[4], (N_DP, N_SECTION, FB, D), FF ** -0.5, 0.0625, ((0, 8), (1, 2), (3, 2)))
    return dict(layer_inputs=layer_inputs, pre_act=pre_act, out_grad=out_grad, w_in=w_in, w_out=w_out)


def gelu_slope(value):
    cdf = 0.5 * (1.0 + lax.erf(value * 0.7071067811865476))
    dens = jnp.exp(-0.5 * value * value) * 0.3989422804014327
    return cdf + value * dens


def rounded(value):
    return lax.optimization_barrier(value.astype(jnp.bfloat16)).astype(jnp.float32)


def reference(layer_inputs, pre_act, out_grad, w_in, w_out):
    in_rows = w_in.reshape(FF, D)
    out_rows = w_out.reshape(FF, D)
    feat = D // N_MP
    units = FF // N_DP
    upper = out_grad
    grad_in = jnp.zeros((FF, D), jnp.float32)
    grad_out = jnp.zeros((FF, D), jnp.float32)
    results = []
    for spot in reversed(range(SECTIONS)):
        back = jnp.zeros((TOKS, FF), jnp.float32)
        for block in range(N_MP):
            piece = jnp.dot(upper[:, block * feat:(block + 1) * feat], out_rows[:, block * feat:(block + 1) * feat].T, preferred_element_type=jnp.float32)
            back = back + rounded(piece)
        saved = pre_act[spot].astype(jnp.float32)
        gee = (back * gelu_slope(saved)).astype(jnp.bfloat16)
        total = upper.astype(jnp.float32)
        for block in range(N_DP):
            piece = jnp.dot(gee[:, block * units:(block + 1) * units], in_rows[block * units:(block + 1) * units, :], preferred_element_type=jnp.float32)
            total = total + rounded(piece)
        result = total.astype(jnp.bfloat16)
        hidden = jax.nn.gelu(saved, approximate=False).astype(jnp.bfloat16)
        grad_in = grad_in + rounded(jnp.dot(gee.T, layer_inputs[spot], preferred_element_type=jnp.float32))
        grad_out = grad_out + rounded(jnp.dot(hidden.T, upper, preferred_element_type=jnp.float32))
        results.append(result)
        upper = result
    in_grads = jnp.stack(results[::-1], axis=0)
    return (in_grads, grad_in.reshape(N_DP, N_SECTION, FB, D), grad_out.reshape(N_DP, N_SECTION, FB, D))
```

```python
import functools

import jax
import jax.numpy as jnp
from jax import lax
from jax.experimental import pallas as pl
from jax.experimental.pallas import tpu as pltpu
from jax.sharding import PartitionSpec as P

MESH = pl.DeviceIdType.MESH
CHUNKS = 2
PIECES = 8
LANES = 128
VMEM_BYTES = 60 * 1024 * 1024


def gelu_cdf(value):
    return 0.5 * (1.0 + lax.erf(value * 0.7071067811865476))


def slope_from(value, cdf):
    dens = jnp.exp(-0.5 * value * value) * 0.3989422804014327
    return cdf + value * dens


def rounded(value):
    return lax.optimization_barrier(value.astype(jnp.bfloat16)).astype(jnp.float32)


def by_tokens(left, right):
    return lax.dot_general(
        left, right, (((0,), (0,)), ((), ())), preferred_element_type=jnp.float32
    )


def by_features(left, right):
    return lax.dot_general(
        left, right, (((1,), (1,)), ((), ())), preferred_element_type=jnp.float32
    )


def exchange_kernel(
    sizes, pre_ref, og_ref, lin_ref, win_hbm, wout_ref,
    res_ref, gee_ref, hid_ref, up_ref, lx_ref,
    win_ref, preb, bp, bq, part, rsp, red, rsz, full,
    load_sem, send_sem, recv_sem,
):
    levels, tok, per = sizes
    rows = tok // CHUNKS
    plane = 4
    s = lax.axis_index("section")
    dp = lax.axis_index("dp")
    m = lax.axis_index("mp")
    z = dp // 2
    y = dp % 2
    p = s * 2 + y

    def at_plane(d):
        s2 = (s + d // 2) % 2
        y2 = (y + d % 2) % 2
        return (s2, z * 2 + y2, m), s2 * 2 + y2

    def at_level(e):
        z2 = (z + e) % levels
        return (s, z2 * 2 + y, m), z2

    load = pltpu.make_async_copy(win_hbm, win_ref, load_sem)
    load.start()

    peers = [at_plane(d)[0] for d in range(1, plane)]
    peers += [at_level(e)[0] for e in range(1, levels)]
    other_core = (s, dp, (m + 1) % 2)
    peers.append(other_core)
    barrier = pltpu.get_barrier_semaphore()
    for peer in peers:
        pl.semaphore_signal(barrier, inc=1, device_id=peer, device_id_type=MESH)
    pl.semaphore_wait(barrier, len(peers))

    started = []

    def send(src, dst, device):
        spot = len(started)
        copy = pltpu.make_async_remote_copy(
            src_ref=src, dst_ref=dst, send_sem=send_sem.at[spot],
            recv_sem=recv_sem.at[spot], device_id=device, device_id_type=MESH,
        )
        copy.start()
        started.append(copy)
        return copy

    x_peer = at_plane(2)[0]
    away = pl.ds(pl.multiple_of((1 - s) * per, per), per)
    mine = pl.ds(pl.multiple_of(s * per, per), per)
    span = [slice(c * rows, (c + 1) * rows) for c in range(CHUNKS)]

    pre_in = [send(pre_ref.at[0, span[c], away], preb.at[c], x_peer) for c in range(CHUNKS)]
    waiting = {}
    piece = tok // PIECES
    pieces = []

    def send_piece():
        i = len(pieces)
        if i < PIECES:
            there = pl.ds(i * piece, piece)
            pieces.append(send(lin_ref.at[0, there, :], lx_ref.at[there, :], x_peer))

    def back(a, c, upper):
        value = by_features(upper, wout_ref[...])
        bp[a, c] = value.astype(jnp.bfloat16)
        waiting[a, c] = [send(bp.at[a, c], bq.at[a, c], other_core)]

    def arrived(a, c):
        for copy in waiting[a, c]:
            copy.wait_recv()

    def hidden_grad(a, c):
        if a == 0:
            pre_in[c].wait_recv()
            if c == 0:
                load.wait()
        arrived(a, c)
        layer = 1 - a
        own = pre_ref[0, span[c], mine]
        saved = jnp.where(s == layer, own, preb[c]).astype(jnp.float32)
        cdf = gelu_cdf(saved)
        total = bp[a, c].astype(jnp.float32) + bq[a, c].astype(jnp.float32)
        gee = (total * slope_from(saved, cdf)).astype(jnp.bfloat16)
        copies = []
        for d in (3, 2, 1, 0):
            device, spot = at_plane(d)
            width = part.shape[-1]
            cols = pl.ds(pl.multiple_of(spot * width, width), width)
            value = jnp.dot(gee, win_ref[:, cols], preferred_element_type=jnp.float32)
            part[a, c, d] = value.astype(jnp.bfloat16)
            if d:
                copies.append(send(part.at[a, c, d], rsp.at[a, c, d], device))
        waiting[a, c] = copies
        gee_ref[(layer + s) % 2, span[c], :] = gee
        hid_ref[a, span[c], :] = (saved * cdf).astype(jnp.bfloat16)

    def reduce_plane(a, c):
        arrived(a, c)
        total = part[a, c, 0].astype(jnp.float32)
        for d in range(1, plane):
            total = total + rsp[a, c, d].astype(jnp.float32)
        total = total.astype(jnp.bfloat16)
        for i in range(levels):
            red[a, c, i] = total[:, i * LANES:(i + 1) * LANES]
        copies = []
        for e in range(1, levels):
            device, spot = at_level(e)
            copies.append(send(red.at[a, c, spot], rsz.at[a, c, e], device))
        waiting[a, c] = copies
        send_piece()

    def reduce_level(a, c):
        arrived(a, c)
        if a == 0:
            cols = pl.ds(pl.multiple_of((p * levels + z) * LANES, LANES), LANES)
            total = og_ref[span[c], cols].astype(jnp.float32)
        else:
            total = full[0, c, p, z].astype(jnp.float32)
        total = total + red[a, c, z].astype(jnp.float32)
        for e in range(1, levels):
            total = total + rsz[a, c, e].astype(jnp.float32)
        full[a, c, p, z] = total.astype(jnp.bfloat16)
        here = full.at[a, c, p, z]
        waiting[a, c] = [send(here, here, at_level(e)[0]) for e in range(1, levels)]
        send_piece()

    def gather_plane(a, c):
        arrived(a, c)
        here = full.at[a, c, p]
        waiting[a, c] = [send(here, here, at_plane(d)[0]) for d in (3, 2, 1)]

    def finish(a, c):
        arrived(a, c)
        value = jnp.concatenate(
            [full[a, c, i, j] for i in range(plane) for j in range(levels)], axis=1
        )
        if a == 0:
            up_ref[span[c], :] = value
            back(1, c, value)
        else:
            res_ref[0, span[c], :] = jnp.where(s == 0, value, up_ref[span[c], :])

    for c in range(CHUNKS):
        back(0, c, og_ref[span[c], :])
    for a in range(2):
        for stage in (hidden_grad, reduce_plane, reduce_level, gather_plane, finish):
            for c in range(CHUNKS):
                stage(a, c)
    while len(pieces) < PIECES:
        send_piece()
    for copy in pieces:
        copy.wait_recv()
    for copy in started:
        copy.wait_send()


def grads_kernel(gee_ref, hid_ref, lin_ref, lx_ref, og_ref, up_ref, gin_ref, gout_ref):
    def term(left, right):
        return by_tokens(left, right).astype(jnp.bfloat16).astype(jnp.float32)

    gin_ref[0, 0] = term(gee_ref[0], lin_ref[0]) + term(gee_ref[1], lx_ref[...])
    gout_ref[0, 0] = term(hid_ref[0], og_ref[...]) + term(hid_ref[1], up_ref[...])


def fused_body(layer_inputs, pre_act, out_grad, w_in, w_out):
    tok, width = out_grad.shape
    per = w_in.shape[2]
    levels = lax.axis_size("dp") // 2
    rows = tok // CHUNKS
    bf = jnp.bfloat16
    slots = 4 + 0 * levels
    copies = CHUNKS * (3 + 2 * (6 + 2 * (levels - 1))) + PIECES
    vmem = pl.BlockSpec(memory_space=pltpu.VMEM)
    anyw = pl.BlockSpec(memory_space=pl.ANY)
    result, gees, hids, upper, other_in = pl.pallas_call(
        functools.partial(exchange_kernel, (levels, tok, per)),
        out_shape=(
            jax.ShapeDtypeStruct((1, tok, width), bf),
            jax.ShapeDtypeStruct((2, tok, per), bf),
            jax.ShapeDtypeStruct((2, tok, per), bf),
            jax.ShapeDtypeStruct((tok, width), bf),
            jax.ShapeDtypeStruct((tok, width), bf),
        ),
        in_specs=[vmem, vmem, anyw, anyw, vmem],
        out_specs=(vmem, vmem, vmem, vmem, anyw),
        scratch_shapes=[
            pltpu.VMEM((per, width), bf),
            pltpu.VMEM((CHUNKS, rows, per), bf),
            pltpu.VMEM((2, CHUNKS, rows, per), bf),
            pltpu.VMEM((2, CHUNKS, rows, per), bf),
            pltpu.VMEM((2, CHUNKS, slots, rows, width // 4), bf),
            pltpu.VMEM((2, CHUNKS, slots, rows, width // 4), bf),
            pltpu.VMEM((2, CHUNKS, levels, rows, LANES), bf),
            pltpu.VMEM((2, CHUNKS, levels, rows, LANES), bf),
            pltpu.VMEM((2, CHUNKS, 4, levels, rows, LANES), bf),
            pltpu.SemaphoreType.DMA,
            pltpu.SemaphoreType.DMA((copies,)),
            pltpu.SemaphoreType.DMA((copies,)),
        ],
        compiler_params=pltpu.CompilerParams(
            collective_id=0, has_side_effects=True, vmem_limit_bytes=VMEM_BYTES
        ),
    )(pre_act, out_grad, layer_inputs, w_in.reshape(per, width), w_out.reshape(per, width))
    tile = min(512, width)
    whole = pl.BlockSpec((2, tok, per), lambda j: (0, 0, 0))
    cols = pl.BlockSpec((tok, tile), lambda j: (0, j))
    grad = pl.BlockSpec((1, 1, per, tile), lambda j: (0, 0, 0, j))
    shape = jax.ShapeDtypeStruct((1, 1, per, width), jnp.float32)
    grad_in, grad_out = pl.pallas_call(
        grads_kernel,
        grid=(width // tile,),
        out_shape=(shape, shape),
        in_specs=[
            whole, whole, pl.BlockSpec((1, tok, tile), lambda j: (0, 0, j)), cols, cols, cols,
        ],
        out_specs=(grad, grad),
    )(gees, hids, layer_inputs, other_in, out_grad, upper)
    return result, grad_in, grad_out


def plain_body(layer_inputs, pre_act, out_grad, w_in, w_out):
    sections = lax.axis_size("section")
    spot = lax.axis_index("section")
    tok, width = out_grad.shape
    per = w_in.shape[2]
    in_rows = w_in.reshape(per, width)
    out_rows = w_out.reshape(per, width)
    blocks = pre_act.reshape(tok, sections, per)
    saved_all = lax.all_to_all(blocks, "section", split_axis=1, concat_axis=0, tiled=True)
    saved_all = saved_all.reshape(sections, tok, per).astype(jnp.float32)
    inputs = lax.all_gather(layer_inputs, "section", axis=0, tiled=True)
    upper = out_grad
    grad_in = jnp.zeros((per, width), jnp.float32)
    grad_out = jnp.zeros((per, width), jnp.float32)
    results = []
    for layer in reversed(range(sections)):
        partial_value = by_features(upper, out_rows).astype(jnp.bfloat16)
        total = lax.psum(partial_value.astype(jnp.float32), "mp")
        saved = saved_all[layer]
        cdf = gelu_cdf(saved)
        gee = (total * slope_from(saved, cdf)).astype(jnp.bfloat16)
        hidden = (saved * cdf).astype(jnp.bfloat16)
        branch = jnp.dot(gee, in_rows, preferred_element_type=jnp.float32)
        branch = lax.psum(branch, ("section", "dp"))
        result = (upper.astype(jnp.float32) + branch).astype(jnp.bfloat16)
        grad_in = grad_in + rounded(by_tokens(gee, inputs[layer]))
        grad_out = grad_out + rounded(by_tokens(hidden, upper))
        results.append(result)
        upper = result
    mine = lax.dynamic_index_in_dim(jnp.stack(results[::-1]), spot, 0, keepdims=True)
    shape = (1, 1, per, width)
    return mine, grad_in.reshape(shape), grad_out.reshape(shape)


def body(layer_inputs, pre_act, out_grad, w_in, w_out):
    tok, width = out_grad.shape
    per = w_in.shape[2]
    groups = lax.axis_size("dp")
    suits = (
        lax.axis_size("section") == 2
        and lax.axis_size("mp") == 2
        and groups % 2 == 0
        and groups > 2
        and width == 2 * groups * LANES
        and per % LANES == 0
        and tok % (CHUNKS * 16) == 0
        and tok % (PIECES * 16) == 0
    )
    chosen = fused_body if suits else plain_body
    return chosen(layer_inputs, pre_act, out_grad, w_in, w_out)


def solution(mesh):
    in_specs = (
        P("section", None, "mp"),
        P("section", None, "dp"),
        P(None, "mp"),
        P("dp", "section", None, "mp"),
        P("dp", "section", None, "mp"),
    )
    out_specs = (
        P("section", None, "mp"),
        P("dp", "section", None, "mp"),
        P("dp", "section", None, "mp"),
    )
    return jax.shard_map(body, mesh=mesh, in_specs=in_specs, out_specs=out_specs, check_vma=False)
```

```python
import functools

import jax
import jax.numpy as jnp
from jax import lax
from jax.experimental import pallas as pl
from jax.experimental.pallas import tpu as pltpu
from jax.sharding import PartitionSpec as P

MESH = pl.DeviceIdType.MESH
CHUNKS = 2
PIECES = CHUNKS
LANES = 128
GRAD_TILE = 512
VMEM_BYTES = 60 * 1024 * 1024


def gelu_cdf(value):
    return 0.5 * (1.0 + lax.erf(value * 0.7071067811865476))


def slope_from(value, cdf):
    dens = jnp.exp(-0.5 * value * value) * 0.3989422804014327
    return cdf + value * dens


def rounded(value):
    return lax.optimization_barrier(value.astype(jnp.bfloat16)).astype(jnp.float32)


def by_tokens(left, right):
    return lax.dot_general(
        left, right, (((0,), (0,)), ((), ())), preferred_element_type=jnp.float32
    )


def by_features(left, right):
    return lax.dot_general(
        left, right, (((1,), (1,)), ((), ())), preferred_element_type=jnp.float32
    )


def exchange_kernel(
    sizes, pre_hbm, og_hbm, lin_ref, win_hbm, wout_hbm,
    res_hbm, gee_hbm, hid_hbm, up_hbm, lx_ref,
    res_ref, gee_ref, hid_ref, up_ref, gee_turned, hid_turned,
    pre_ref, og_ref, win_ref, wout_ref, preb, bp, bq, part, rsp, red, rsz, full,
    load_sem, store_sem, send_sem, recv_sem,
):
    levels, tok, per = sizes
    rows = tok // CHUNKS
    plane = 4
    s = lax.axis_index("section")
    dp = lax.axis_index("dp")
    m = lax.axis_index("mp")
    z = dp // 2
    y = dp % 2
    p = s * 2 + y

    def at_plane(d):
        s2 = (s + d // 2) % 2
        y2 = (y + d % 2) % 2
        return (s2, z * 2 + y2, m), s2 * 2 + y2

    def at_level(e):
        z2 = (z + e) % levels
        return (s, z2 * 2 + y, m), z2

    peers = [at_plane(d)[0] for d in range(1, plane)]
    peers += [at_level(e)[0] for e in range(1, levels)]
    other_core = (s, dp, (m + 1) % 2)
    peers.append(other_core)
    barrier = pltpu.get_barrier_semaphore()
    for peer in peers:
        pl.semaphore_signal(barrier, inc=1, device_id=peer, device_id_type=MESH)

    pairs = ((og_hbm, og_ref), (wout_hbm, wout_ref), (pre_hbm, pre_ref), (win_hbm, win_ref))
    loads = [
        pltpu.make_async_copy(src, dst, load_sem.at[i]) for i, (src, dst) in enumerate(pairs)
    ]
    for load in loads:
        load.start()

    started = []
    stores = []

    def store(src, dst):
        copy = pltpu.make_async_copy(src, dst, store_sem.at[len(stores)])
        copy.start()
        stores.append(copy)

    def send(src, dst, device):
        spot = len(started)
        copy = pltpu.make_async_remote_copy(
            src_ref=src, dst_ref=dst, send_sem=send_sem.at[spot],
            recv_sem=recv_sem.at[spot], device_id=device, device_id_type=MESH,
        )
        copy.start()
        started.append(copy)
        return copy

    x_peer = at_plane(2)[0]
    away = pl.ds(pl.multiple_of((1 - s) * per, per), per)
    mine = pl.ds(pl.multiple_of(s * per, per), per)
    span = [slice(c * rows, (c + 1) * rows) for c in range(CHUNKS)]
    waiting = {}
    piece = tok // (PIECES * levels)
    pieces = []
    relays = []

    def send_piece(a):
        i = len(pieces) if a == 0 else len(relays)
        if i >= PIECES:
            return
        begin = pl.multiple_of((z * PIECES + i) * piece, piece)
        there = lx_ref.at[pl.ds(begin, piece), :]
        if a == 0:
            pieces.append(send(lin_ref.at[0, pl.ds(begin, piece), :], there, x_peer))
        else:
            pieces[i].wait_recv()
            relays.append([send(there, there, at_level(e)[0]) for e in range(1, levels)])

    def multiply(a, c, upper):
        bp[a, c] = by_features(upper, wout_ref[...]).astype(jnp.bfloat16)

    def back(a, c):
        waiting[a, c] = [send(bp.at[a, c], bq.at[a, c], other_core)]

    def arrived(a, c):
        for copy in waiting[a, c]:
            copy.wait_recv()

    def hidden_grad(a, c):
        if a == 0:
            pre_in[c].wait_recv()
            if c == 0:
                loads[3].wait()
        arrived(a, c)
        layer = 1 - a
        own = pre_ref[0, span[c], mine]
        saved = jnp.where(s == layer, own, preb[c]).astype(jnp.float32)
        cdf = gelu_cdf(saved)
        total = bp[a, c].astype(jnp.float32) + bq[a, c].astype(jnp.float32)
        gee = (total * slope_from(saved, cdf)).astype(jnp.bfloat16)
        copies = []
        for d in (3, 2, 1, 0):
            device, spot = at_plane(d)
            width = part.shape[-1]
            cols = pl.ds(pl.multiple_of(spot * width, width), width)
            value = jnp.dot(gee, win_ref[:, cols], preferred_element_type=jnp.float32)
            part[a, c, d] = value.astype(jnp.bfloat16)
            if d:
                copies.append(send(part.at[a, c, d], rsp.at[a, c, d], device))
        waiting[a, c] = copies
        place = pl.multiple_of(((layer + s) % 2) * tok + c * rows, rows)
        gee_ref[pl.ds(place, rows), :] = gee
        hid_ref[pl.ds(a * tok + c * rows, rows), :] = (saved * cdf).astype(jnp.bfloat16)

    def reduce_plane(a, c):
        arrived(a, c)
        total = part[a, c, 0].astype(jnp.float32)
        for d in range(1, plane):
            total = total + rsp[a, c, d].astype(jnp.float32)
        total = total.astype(jnp.bfloat16)
        for i in range(levels):
            red[a, c, i] = total[:, i * LANES:(i + 1) * LANES]
        copies = []
        for e in range(1, levels):
            device, spot = at_level(e)
            copies.append(send(red.at[a, c, spot], rsz.at[a, c, e], device))
        waiting[a, c] = copies
        if a == 1 and c == CHUNKS - 1:
            gee_turned[...] = gee_ref[...].T
            store(gee_turned, gee_hbm)
            hid_turned[...] = hid_ref[...].T
            store(hid_turned, hid_hbm)

    def reduce_level(a, c):
        arrived(a, c)
        if a == 0:
            cols = pl.ds(pl.multiple_of((p * levels + z) * LANES, LANES), LANES)
            total = og_ref[span[c], cols].astype(jnp.float32)
        else:
            total = full[0, c, p, z].astype(jnp.float32)
        total = total + red[a, c, z].astype(jnp.float32)
        for e in range(1, levels):
            total = total + rsz[a, c, e].astype(jnp.float32)
        full[a, c, p, z] = total.astype(jnp.bfloat16)
        here = full.at[a, c, p, z]
        waiting[a, c] = [send(here, here, at_level(e)[0]) for e in range(1, levels)]
        if a == 0:
            send_piece(0)

    def gather_plane(a, c):
        arrived(a, c)
        here = full.at[a, c, p]
        waiting[a, c] = [send(here, here, at_plane(d)[0]) for d in (3, 2, 1)]

    def finish(a, c):
        arrived(a, c)
        value = jnp.concatenate(
            [full[a, c, i, j] for i in range(plane) for j in range(levels)], axis=1
        )
        if a == 0:
            up_ref[span[c], :] = value
            multiply(1, c, value)
            back(1, c)
            store(up_ref.at[span[c]], up_hbm.at[span[c]])
            send_piece(1)
        else:
            res_ref[span[c], :] = jnp.where(s == 0, value, up_ref[span[c], :])
            store(res_ref.at[span[c]], res_hbm.at[span[c]])

    loads[0].wait()
    loads[1].wait()
    multiply(0, 0, og_ref[span[0], :])
    loads[2].wait()
    pl.semaphore_wait(barrier, len(peers))
    pre_in = [send(pre_ref.at[0, span[c], away], preb.at[c], x_peer) for c in range(CHUNKS)]
    back(0, 0)
    for c in range(1, CHUNKS):
        multiply(0, c, og_ref[span[c], :])
        back(0, c)
    for a in range(2):
        for stage in (hidden_grad, reduce_plane, reduce_level, gather_plane, finish):
            for c in range(CHUNKS):
                stage(a, c)
    for copies in relays:
        for copy in copies:
            copy.wait_recv()
    for copy in started:
        copy.wait_send()
    for copy in stores:
        copy.wait()


def grads_kernel(
    gee_hbm, hid_hbm, lin_hbm, lx_hbm, og_hbm, up_hbm, given_hbm,
    res_hbm, gin_hbm, gout_hbm,
    gee, hid, inputs, uppers, given, gin, gout, load_sem, store_sem,
):
    tok, width = og_hbm.shape
    tile = min(GRAD_TILE, width)
    pairs = (
        (hid_hbm, hid), (og_hbm, uppers.at[:tok]), (up_hbm, uppers.at[tok:]),
        (gee_hbm, gee), (lin_hbm.at[0], inputs.at[:tok]), (lx_hbm, inputs.at[tok:]),
        (given_hbm, given),
    )
    loads = [
        pltpu.make_async_copy(src, dst, load_sem.at[i]) for i, (src, dst) in enumerate(pairs)
    ]
    for load in loads:
        load.start()
    stores = []

    def store(src, dst):
        copy = pltpu.make_async_copy(src, dst, store_sem.at[len(stores)])
        copy.start()
        stores.append(copy)

    sides = ((0, hid, uppers, gout, gout_hbm), (3, gee, inputs, gin, gin_hbm))
    for first, left, right, held, out in sides:
        for load in loads[first:first + 3]:
            load.wait()
        for t in range(width // tile):
            cols = slice(t * tile, (t + 1) * tile)
            held[:, cols] = jnp.dot(
                left[...], right[:, cols], preferred_element_type=jnp.float32
            )
            store(held.at[:, cols], out.at[0, 0, :, cols])
    loads[6].wait()
    store(given, res_hbm.at[0])
    for copy in stores:
        copy.wait()


def fused_body(layer_inputs, pre_act, out_grad, w_in, w_out):
    tok, width = out_grad.shape
    per = w_in.shape[2]
    levels = lax.axis_size("dp") // 2
    rows = tok // CHUNKS
    bf = jnp.bfloat16
    copies = CHUNKS * (3 + 2 * (6 + 2 * (levels - 1))) + PIECES * levels
    anyw = pl.BlockSpec(memory_space=pl.ANY)
    result, gees, hids, upper, other_in = pl.pallas_call(
        functools.partial(exchange_kernel, (levels, tok, per)),
        out_shape=(
            jax.ShapeDtypeStruct((tok, width), bf),
            jax.ShapeDtypeStruct((per, 2 * tok), bf),
            jax.ShapeDtypeStruct((per, 2 * tok), bf),
            jax.ShapeDtypeStruct((tok, width), bf),
            jax.ShapeDtypeStruct((tok, width), bf),
        ),
        in_specs=[anyw] * 5,
        out_specs=[anyw] * 5,
        scratch_shapes=[
            pltpu.VMEM((tok, width), bf),
            pltpu.VMEM((2 * tok, per), bf),
            pltpu.VMEM((2 * tok, per), bf),
            pltpu.VMEM((tok, width), bf),
            pltpu.VMEM((per, 2 * tok), bf),
            pltpu.VMEM((per, 2 * tok), bf),
            pltpu.VMEM(pre_act.shape, bf),
            pltpu.VMEM((tok, width), bf),
            pltpu.VMEM((per, width), bf),
            pltpu.VMEM((per, width), bf),
            pltpu.VMEM((CHUNKS, rows, per), bf),
            pltpu.VMEM((2, CHUNKS, rows, per), bf),
            pltpu.VMEM((2, CHUNKS, rows, per), bf),
            pltpu.VMEM((2, CHUNKS, 4, rows, width // 4), bf),
            pltpu.VMEM((2, CHUNKS, 4, rows, width // 4), bf),
            pltpu.VMEM((2, CHUNKS, levels, rows, LANES), bf),
            pltpu.VMEM((2, CHUNKS, levels, rows, LANES), bf),
            pltpu.VMEM((2, CHUNKS, 4, levels, rows, LANES), bf),
            pltpu.SemaphoreType.DMA((4,)),
            pltpu.SemaphoreType.DMA((2 * CHUNKS + 2,)),
            pltpu.SemaphoreType.DMA((copies,)),
            pltpu.SemaphoreType.DMA((copies,)),
        ],
        compiler_params=pltpu.CompilerParams(
            collective_id=0, has_side_effects=True, vmem_limit_bytes=VMEM_BYTES
        ),
    )(pre_act, out_grad, layer_inputs, w_in.reshape(per, width), w_out.reshape(per, width))
    tiles = width // min(GRAD_TILE, width)
    shape = jax.ShapeDtypeStruct((1, 1, per, width), jnp.float32)
    return pl.pallas_call(
        grads_kernel,
        out_shape=(jax.ShapeDtypeStruct((1, tok, width), bf), shape, shape),
        in_specs=[anyw] * 7,
        out_specs=[anyw] * 3,
        scratch_shapes=[
            pltpu.VMEM((per, 2 * tok), bf),
            pltpu.VMEM((per, 2 * tok), bf),
            pltpu.VMEM((2 * tok, width), bf),
            pltpu.VMEM((2 * tok, width), bf),
            pltpu.VMEM((tok, width), bf),
            pltpu.VMEM((per, width), jnp.float32),
            pltpu.VMEM((per, width), jnp.float32),
            pltpu.SemaphoreType.DMA((7,)),
            pltpu.SemaphoreType.DMA((2 * tiles + 1,)),
        ],
        compiler_params=pltpu.CompilerParams(vmem_limit_bytes=VMEM_BYTES),
    )(gees, hids, layer_inputs, other_in, out_grad, upper, result)


def plain_body(layer_inputs, pre_act, out_grad, w_in, w_out):
    sections = lax.axis_size("section")
    spot = lax.axis_index("section")
    tok, width = out_grad.shape
    per = w_in.shape[2]
    in_rows = w_in.reshape(per, width)
    out_rows = w_out.reshape(per, width)
    blocks = pre_act.reshape(tok, sections, per)
    saved_all = lax.all_to_all(blocks, "section", split_axis=1, concat_axis=0, tiled=True)
    saved_all = saved_all.reshape(sections, tok, per).astype(jnp.float32)
    inputs = lax.all_gather(layer_inputs, "section", axis=0, tiled=True)
    upper = out_grad
    grad_in = jnp.zeros((per, width), jnp.float32)
    grad_out = jnp.zeros((per, width), jnp.float32)
    results = []
    for layer in reversed(range(sections)):
        partial_value = by_features(upper, out_rows).astype(jnp.bfloat16)
        total = lax.psum(partial_value.astype(jnp.float32), "mp")
        saved = saved_all[layer]
        cdf = gelu_cdf(saved)
        gee = (total * slope_from(saved, cdf)).astype(jnp.bfloat16)
        hidden = (saved * cdf).astype(jnp.bfloat16)
        branch = jnp.dot(gee, in_rows, preferred_element_type=jnp.float32)
        branch = lax.psum(branch, ("section", "dp"))
        result = (upper.astype(jnp.float32) + branch).astype(jnp.bfloat16)
        grad_in = grad_in + rounded(by_tokens(gee, inputs[layer]))
        grad_out = grad_out + rounded(by_tokens(hidden, upper))
        results.append(result)
        upper = result
    mine = lax.dynamic_index_in_dim(jnp.stack(results[::-1]), spot, 0, keepdims=True)
    shape = (1, 1, per, width)
    return mine, grad_in.reshape(shape), grad_out.reshape(shape)


def body(layer_inputs, pre_act, out_grad, w_in, w_out):
    tok, width = out_grad.shape
    per = w_in.shape[2]
    groups = lax.axis_size("dp")
    suits = (
        lax.axis_size("section") == 2
        and lax.axis_size("mp") == 2
        and groups % 2 == 0
        and groups > 2
        and width == 2 * groups * LANES
        and per % LANES == 0
        and tok % (CHUNKS * 16) == 0
        and tok % (PIECES * groups * 8) == 0
    )
    chosen = fused_body if suits else plain_body
    return chosen(layer_inputs, pre_act, out_grad, w_in, w_out)


def solution(mesh):
    in_specs = (
        P("section", None, "mp"),
        P("section", None, "dp"),
        P(None, "mp"),
        P("dp", "section", None, "mp"),
        P("dp", "section", None, "mp"),
    )
    out_specs = (
        P("section", None, "mp"),
        P("dp", "section", None, "mp"),
        P("dp", "section", None, "mp"),
    )
    return jax.shard_map(body, mesh=mesh, in_specs=in_specs, out_specs=out_specs, check_vma=False)
```
